32 devices in a mesh: rep: 4 (over x, y), dp: 8 (over z, core).
Axes of the slice: x: 2, y: 2, z: 4, core: 2. Of those that a mesh axis runs over, the one named last changes fastest.
Arguments:
- x: bfloat16 [32, 2048, 640], P(('rep', 'dp')), parts along dimension 0
- dy: bfloat16 [32, 2048, 640], P(('rep', 'dp')), parts along dimension 0
- wq: bfloat16 [2, 640, 512], P(None, 'dp')
- wk: bfloat16 [2, 640, 256], P(None, 'dp')
- wv: bfloat16 [2, 640, 256], P(None, 'dp')
- wo: bfloat16 [2, 512, 640], P(None, 'dp')
- w_gate: bfloat16 [2, 640, 2560], P(None, 'dp')
- w_up: bfloat16 [2, 640, 2560], P(None, 'dp')
- w_down: bfloat16 [2, 2560, 640], P(None, 'dp')
- m_wq: float32 [2, 640, 512], P(None, 'dp')
- m_wk: float32 [2, 640, 256], P(None, 'dp')
- m_wv: float32 [2, 640, 256], P(None, 'dp')
- m_wo: float32 [2, 512, 640], P(None, 'dp')
- m_w_gate: float32 [2, 640, 2560], P(None, 'dp')
- m_w_up: float32 [2, 640, 2560], P(None, 'dp')
- m_w_down: float32 [2, 2560, 640], P(None, 'dp')
- v_wq: float32 [2, 640, 512], P(None, 'dp')
- v_wk: float32 [2, 640, 256], P(None, 'dp')
- v_wv: float32 [2, 640, 256], P(None, 'dp')
- v_wo: float32 [2, 512, 640], P(None, 'dp')
- v_w_gate: float32 [2, 640, 2560], P(None, 'dp')
- v_w_up: float32 [2, 640, 2560], P(None, 'dp')
- v_w_down: float32 [2, 2560, 640], P(None, 'dp')
Outputs:
- output 1: bfloat16 [8, 640, 512], P('rep', 'dp'), parts along dimension 0
- output 2: bfloat16 [8, 640, 256], P('rep', 'dp'), parts along dimension 0
- output 3: bfloat16 [8, 640, 256], P('rep', 'dp'), parts along dimension 0
- output 4: bfloat16 [8, 512, 640], P('rep', 'dp'), parts along dimension 0
- output 5: bfloat16 [8, 640, 2560], P('rep', 'dp'), parts along dimension 0
- output 6: bfloat16 [8, 640, 2560], P('rep', 'dp'), parts along dimension 0
- output 7: bfloat16 [8, 2560, 640], P('rep', 'dp'), parts along dimension 0
- output 8: float32 [8, 640, 512], P('rep', 'dp'), parts along dimension 0
- output 9: float32 [8, 640, 256], P('rep', 'dp'), parts along dimension 0
- output 10: float32 [8, 640, 256], P('rep', 'dp'), parts along dimension 0
- output 11: float32 [8, 512, 640], P('rep', 'dp'), parts along dimension 0
- output 12: float32 [8, 640, 2560], P('rep', 'dp'), parts along dimension 0
- output 13: float32 [8, 640, 2560], P('rep', 'dp'), parts along dimension 0
- output 14: float32 [8, 2560, 640], P('rep', 'dp'), parts along dimension 0
- output 15: float32 [8, 640, 512], P('rep', 'dp'), parts along dimension 0
- output 16: float32 [8, 640, 256], P('rep', 'dp'), parts along dimension 0
- output 17: float32 [8, 640, 256], P('rep', 'dp'), parts along dimension 0
- output 18: float32 [8, 512, 640], P('rep', 'dp'), parts along dimension 0
- output 19: float32 [8, 640, 2560], P('rep', 'dp'), parts along dimension 0
- output 20: float32 [8, 640, 2560], P('rep', 'dp'), parts along dimension 0
- output 21: float32 [8, 2560, 640], P('rep', 'dp'), parts along dimension 0
There are 4 independent parts. The reference program is written for one: setup_inputs(seed, part) draws one part's arguments, and reference() takes and returns one part's arrays. A program takes and returns all parts, laid end to end along the dimension named above; an argument that names none is the same for every part.
All inputs are finite; a program needn't handle non-finite values.
Results may differ from the reference program's by a relative error of at most 0.034.
Values are sent between devices in bfloat16 or wider.
A program may use at most 2 GiB of HBM per device.

```python
import jax
import jax.numpy as jnp
from jax import lax

SEQUENCES = 8
TOKENS = 2048
D = 640
HEADS = 2
KV_HEADS = 1
HEAD = 256
FF = 2560
LAYERS = 2
THETA = 10000
NAMES = ("wq", "wk", "wv", "wo", "w_gate", "w_up", "w_down")
SHAPES = {
    "wq": (LAYERS, D, HEADS * HEAD),
    "wk": (LAYERS, D, KV_HEADS * HEAD),
    "wv": (LAYERS, D, KV_HEADS * HEAD),
    "wo": (LAYERS, HEADS * HEAD, D),
    "w_gate": (LAYERS, D, FF),
    "w_up": (LAYERS, D, FF),
    "w_down": (LAYERS, FF, D),
}


def bump(key, n, height):
    away = (jnp.arange(n, dtype=jnp.int32) - jax.random.randint(key, (), 0, n, jnp.int32)) % n
    return jnp.where(away < n // 8, height, 1.0)


def together(key, own, strength):
    shared = jax.random.normal(key, own.shape[1:], jnp.float32)
    return (own + strength * shared) * lax.rsqrt(1 + strength * strength)


def setup_inputs(seed: int = 0, part: int = 0) -> dict:
    kx, kdy, ka, kb, kz, kf, kh, kl, *keys = jax.random.split(jax.random.key(seed), 8 + 3 * len(NAMES))
    kx, kdy, ka, kb = (jax.random.fold_in(k, part) for k in (kx, kdy, ka, kb))
    kw, km, kv = (keys[i::3] for i in range(3))
    shape = (SEQUENCES, TOKENS, D)
    much_x, much_dy = jax.random.uniform(kz, (2,), jnp.float32, 0.0, 1.0)
    loud = 2.0 ** jax.random.uniform(jax.random.fold_in(kz, 1), (), jnp.float32, -1.0, 2.0)
    layers = 2.0 ** jax.random.uniform(kl, (LAYERS, 1, 1), jnp.float32, -1.0, 1.0)
    times = {"wq": 1.0, "wk": 1.0, "wv": 2.0, "wo": layers, "w_gate": 1.0, "w_up": bump(kh, FF, 4.0), "w_down": layers}
    x = together(ka, jax.random.normal(kx, shape, jnp.float32), much_x) * bump(kf, D, 4.0)
    dy = together(kb, jax.random.normal(kdy, shape, jnp.float32), much_dy)
    drawn = {"x": x.astype(jnp.bfloat16), "dy": (loud * dy * (SEQUENCES * TOKENS) ** -0.5).astype(jnp.bfloat16)}
    for key, name in zip(kw, NAMES, strict=True):
        drawn[name] = (jax.random.normal(key, SHAPES[name], jnp.float32) * SHAPES[name][1] ** -0.5 * times[name]).astype(jnp.bfloat16)
    for key, name in zip(km, NAMES, strict=True):
        drawn[f"m_{name}"] = 0.1 * jax.random.normal(key, SHAPES[name], jnp.float32)
    for key, name in zip(kv, NAMES, strict=True):
        drawn[f"v_{name}"] = loud * loud * jax.random.uniform(key, SHAPES[name], jnp.float32, 0.2, 0.6)
    return drawn


def matmul(a, w):
    return jnp.dot(a, w, preferred_element_type=jnp.float32).astype(jnp.bfloat16)


def normed(h):
    wide = h.astype(jnp.float32)
    scale = lax.rsqrt(jnp.mean(wide**2, -1, keepdims=True) + 1e-6)
    return (wide * scale).astype(jnp.bfloat16)


def turned(t, theta):
    half = t.shape[-1] // 2
    angle = jnp.arange(t.shape[0], dtype=jnp.float32)[:, None] * theta ** (-jnp.arange(half, dtype=jnp.float32) / half)
    cos, sin = jnp.cos(angle)[:, None], jnp.sin(angle)[:, None]
    a, b = t[..., :half].astype(jnp.float32), t[..., half:].astype(jnp.float32)
    return jnp.concatenate([a * cos - b * sin, b * cos + a * sin], -1).astype(jnp.bfloat16)


def seen_by(q, k, v):
    tokens, kv = q.shape[0], k.shape[1]
    q = q.reshape(tokens, kv, -1, q.shape[-1])
    scores = jnp.einsum("tgsd,ugd->gstu", q.astype(jnp.float32), k.astype(jnp.float32)) * q.shape[-1] ** -0.5
    place = jnp.arange(tokens)
    weights = jax.nn.softmax(jnp.where(place[:, None] >= place, scores, -jnp.inf), -1).astype(jnp.bfloat16)
    return jnp.einsum("gstu,ugd->tgsd", weights.astype(jnp.float32), v.astype(jnp.float32)).astype(jnp.bfloat16).reshape(tokens, -1)


def layer(h, w):
    a = normed(h)
    q, k = (turned(matmul(a, w[name]).reshape(h.shape[0], -1, HEAD), THETA) for name in ("wq", "wk"))
    h = h + matmul(seen_by(q, k, matmul(a, w["wv"]).reshape(h.shape[0], -1, HEAD)), w["wo"])
    b = normed(h)
    gate = jnp.dot(b, w["w_gate"], preferred_element_type=jnp.float32)
    up = jnp.dot(b, w["w_up"], preferred_element_type=jnp.float32)
    return h + matmul((jax.nn.silu(gate) * up).astype(jnp.bfloat16), w["w_down"])


def adamw(w, m, v, g):
    m = 0.9 * m + 0.1 * g
    v = 0.95 * v + 0.05 * g * g
    step = m * lax.rsqrt(v + 1e-8) + 0.1 * w
    return (w - 0.02 * step).astype(jnp.bfloat16), m, v


def stack(weights, h):
    return lax.scan(lambda h, w: (layer(h, w), None), h, weights)[0]


def reference(x, dy, wq, wk, wv, wo, w_gate, w_up, w_down, m_wq, m_wk, m_wv, m_wo, m_w_gate, m_w_up, m_w_down, v_wq, v_wk, v_wv, v_wo, v_w_gate, v_w_up, v_w_down):
    weights = dict(zip(NAMES, (wq, wk, wv, wo, w_gate, w_up, w_down), strict=True))

    def take(so_far, sequence):
        h, by_y = sequence
        _, back = jax.vjp(stack, weights, h)
        by_weights, by_h = back(by_y)
        return jax.tree.map(lambda total, term: total + term.astype(jnp.float32), so_far, by_weights), by_h

    none_yet = {name: jnp.zeros(w.shape, jnp.float32) for name, w in weights.items()}
    by_weights, by_x = lax.scan(take, none_yet, (x, dy))
    gradients = [by_weights[name].astype(jnp.bfloat16).astype(jnp.float32) for name in NAMES]
    first = (m_wq, m_wk, m_wv, m_wo, m_w_gate, m_w_up, m_w_down)
    second = (v_wq, v_wk, v_wv, v_wo, v_w_gate, v_w_up, v_w_down)
    new = [adamw(weights[name].astype(jnp.float32), m, v, g) for name, m, v, g in zip(NAMES, first, second, gradients, strict=True)]
    return tuple(one[which] for which in range(3) for one in new)
```

```python
import functools

import jax
import jax.numpy as jnp
from jax import lax
from jax.experimental import pallas as pl
from jax.experimental.pallas import tpu as pltpu
from jax.sharding import PartitionSpec as P

HEAD = 256
HEADS = range(2)
PAIR = 2 * HEAD
HALF = HEAD // 2
THETA = 10000
FB = 512
RT = 512
CHIPS = 4
ONES = 16
NEG = -1e30
HIDDEN = 2 * NEG
LOG2E = 1.4426950408889634
SCALE = HEAD**-0.5
TEMPER = SCALE * LOG2E
VMEM = 67043328
BF = jnp.bfloat16
F32 = jnp.float32
ANY = pl.BlockSpec(memory_space=pl.ANY)
WHOLE = pl.BlockSpec(memory_space=pltpu.VMEM)


def _dot(a, b, ca, cb):
    return lax.dot_general(a, b, (((ca,), (cb,)), ((), ())), preferred_element_type=F32)


def mm(a, b):
    return _dot(a, b, 1, 0)


def mt(a, b):
    return _dot(a, b, 1, 1)


def tm(a, b):
    return _dot(a, b, 0, 0)


def shape(dtype, *dims):
    return jax.ShapeDtypeStruct(dims, dtype)


def vm(dtype, *dims):
    return pltpu.VMEM(dims, dtype)


def dma(*dims):
    return pltpu.SemaphoreType.DMA(dims)


def loop(n, do, first=0):
    def body(i, kept):
        do(i)
        return kept

    lax.fori_loop(first, n, body, first)


def span(i, size):
    return pl.ds(pl.multiple_of(i * size, size), size)


def rows(at, size):
    return pl.ds(pl.multiple_of(at, 8), size)


def lane(m):
    return slice(m * HEAD, (m + 1) * HEAD)


def at_step(i, n, *todo):
    @pl.when(i == n)
    def _():
        for do, *given in todo:
            do(*given)


def remote(src, dst, send, recv, to):
    return pltpu.make_async_remote_copy(src_ref=src, dst_ref=dst, send_sem=send, recv_sem=recv, device_id=to, device_id_type=pl.DeviceIdType.MESH)


def signal(sem, to):
    pl.semaphore_signal(sem, inc=1, device_id=to, device_id_type=pl.DeviceIdType.MESH)


def rms(wide):
    return lax.rsqrt(jnp.mean(wide * wide, -1, keepdims=True) + 1e-6)


def normed(h):
    wide = h.astype(F32)
    return (wide * rms(wide)).astype(BF)


def normed_back(h, ct):
    wide = h.astype(F32)
    s = rms(wide)
    along = jnp.sum(ct * wide, -1, keepdims=True) * (s * s * s) * (1 / h.shape[-1])
    return (ct * s - wide * along).astype(BF).astype(F32)


def turn(t, cos, sin):
    t = t.astype(F32)
    a, b = t[:, :HALF], t[:, HALF:]
    return jnp.concatenate([a * cos - b * sin, b * cos + a * sin], -1).astype(BF)


def turn_back(t, cos, sin):
    return turn(t, cos, -sin)


def sigmoid(x):
    return 1 / (1 + jnp.exp(-x))


def causal(size):
    return lax.broadcasted_iota(jnp.int32, (size, size), 1) >= lax.broadcasted_iota(jnp.int32, (size, size), 0)


class Fetch:
    def __init__(self, items, sems):
        self.items = items
        (self.here, self.z_send, self.z_recv, self.x_send, self.x_recv, self.y_send, self.y_recv, self.xd_send, self.xd_recv, self.yd_send,
         self.yd_recv, self.c_send, self.c_recv, self.own_send, self.own_recv) = sems
        self.rep, self.dp = lax.axis_index("rep"), lax.axis_index("dp")
        self.z, self.c = self.dp // 2, self.dp % 2
        x, y = self.rep // 2, self.rep % 2
        self.rx, self.ry, self.rd = (1 - x) * 2 + y, x * 2 + (1 - y), (1 - x) * 2 + (1 - y)
        self.to_x, self.to_y, self.to_core = (self.rx, self.dp), (self.ry, self.dp), (self.rep, self.z * 2 + (1 - self.c))

    def up(self, k):
        return lax.rem(self.z + k, CHIPS)

    def peers(self):
        return [self.to_x, self.to_y, self.to_core] + [(self.rep, self.up(k) * 2 + self.c) for k in range(1, CHIPS)]

    def quarter(self, n, base, r, half=None):
        own, ref, columns = self.items[n]
        size, width = own.shape
        if columns:
            across = span(r, width // CHIPS)
        else:
            across = slice(None)
            size = size // CHIPS
            base = base + r * size
        if half is not None:
            size = size // 2
            base = base + half * size
        return rows(base, size), across

    def place(self, n, d, r, half=None):
        return self.items[n][1].at[self.quarter(n, d * self.items[n][0].shape[0], r, half)]

    def block(self, n, d):
        size = self.items[n][0].shape[0]
        return self.items[n][1].at[rows(d * size, size)]

    def mine(self, n, k):
        src = self.items[n][0].at[self.quarter(n, 0, self.rep)]
        return remote(src, self.place(n, self.dp, self.rep), self.z_send.at[n, k - 1], self.z_recv.at[n, self.z], (self.rep, self.up(k) * 2 + self.c))

    def own(self, n):
        return remote(self.items[n][0], self.block(n, self.dp), self.own_send.at[n], self.own_recv.at[n], self.to_core)

    def stay(self, n):
        return pltpu.make_async_copy(self.items[n][0], self.block(n, self.dp), self.here.at[n])

    def hop(self, n, s, how, d=None):
        d = s * 2 + self.c if d is None else d
        r, half, send, recv, to = {
            "z": (self.rep, None, self.z_send, self.z_recv, self.to_x),
            "x": (self.rep, None, self.x_send, self.x_recv, self.to_x),
            "y": (self.rep, None, self.y_send, self.y_recv, self.to_y),
            "from x": (self.rx, None, self.x_send, self.x_recv, self.to_x),
            "from y": (self.ry, None, self.y_send, self.y_recv, self.to_y),
            "x on": (self.rx, 0, self.yd_send, self.yd_recv, self.to_y),
            "y on": (self.ry, 1, self.xd_send, self.xd_recv, self.to_x),
            "from x on": (self.rd, 0, self.yd_send, self.yd_recv, self.to_y),
            "from y on": (self.rd, 1, self.xd_send, self.xd_recv, self.to_x),
        }[how]
        ref = self.place(n, d, r, half)
        return remote(ref, ref, send.at[n, 0 if how == "z" else s], recv.at[n, s], to)

    def pieces(self):
        return enumerate(((self.rep, None), (self.rx, None), (self.ry, None), (self.rd, 0), (self.rd, 1)))

    def core(self, n, s, i, other=False):
        r, half = dict(self.pieces())[i]
        ref = self.place(n, s * 2 + (1 - self.c if other else self.c), r, half)
        return remote(ref, ref, self.c_send.at[n, s, i], self.c_recv.at[n, s, i], self.to_core)

    def each(self, do):
        loop(CHIPS, lambda k: do(self.up(k)), 1)

    def begin(self, barrier):
        peers = self.peers()
        for peer in peers:
            signal(barrier, peer)
        pl.semaphore_wait(barrier, len(peers))
        for n in range(len(self.items)):
            loop(CHIPS, lambda k: self.mine(n, k).start(), 1)
        for n in range(len(self.items)):
            self.own(n).start()
            self.stay(n).start()

    def on_z(self, n):
        def one(s):
            self.hop(n, s, "z").wait_recv()
            self.hop(n, s, "x").start()
            self.hop(n, s, "y").start()
            self.core(n, s, 0).start()

        self.each(one)

    def on_xy(self, n):
        def one(s):
            self.hop(n, s, "from x").wait_recv()
            self.hop(n, s, "x on").start()
            self.core(n, s, 1).start()
            self.hop(n, s, "from y").wait_recv()
            self.hop(n, s, "y on").start()
            self.core(n, s, 2).start()

        self.each(one)

    def on_diagonal(self, n):
        def one(s):
            self.hop(n, s, "from x on").wait_recv()
            self.core(n, s, 3).start()
            self.hop(n, s, "from y on").wait_recv()
            self.core(n, s, 4).start()

        self.each(one)

    def ready(self, n):
        self.stay(n).wait()
        ref = self.block(n, self.z * 2 + (1 - self.c))
        remote(ref, ref, self.own_send.at[n], self.own_recv.at[n], self.to_core).wait_recv()

        def one(s):
            for i, _ in self.pieces():
                self.core(n, s, i, True).wait_recv()

        self.each(one)

    def sent(self, n):
        self.own(n).wait_send()
        loop(CHIPS, lambda k: self.mine(n, k).wait_send(), 1)

        def one(s):
            for how in ("x", "y", "x on", "y on"):
                self.hop(n, s, how).wait_send()
            for i, _ in self.pieces():
                self.core(n, s, i).wait_send()

        self.each(one)


def fetch_sems(n):
    return [dma(n), dma(n, CHIPS - 1)] + [dma(n, CHIPS)] * 9 + [dma(n, CHIPS, 5)] * 2 + [dma(n)] * 2


def forward_kernel(*refs, layers):
    it = iter(refs)
    take = lambda n: [next(it) for _ in range(n)]
    x, qkv, wo, gate, up, down, cos, sin = take(8)
    o_qkv, o_wo, o_gu, o_down, o_h, o_mid, o_q, o_k, o_v, o_o, o_lse = take(11)
    h_s, mid_s, q_s, k_s, v_s, vt_s, o_s, lse_s, top_s, mix_s, act_s, wqkv_s, wo_s, wgu_s, wd_s, load_sem, out_sem = take(17)
    sems = take(15)
    t = h_s.shape[0]
    f = wd_s.shape[0]
    items = []
    for l in range(layers):
        items += [(qkv.at[l], o_qkv.at[l], True), (wo.at[l], o_wo.at[l], False), (gate.at[l], o_gu.at[l, 0], True), (up.at[l], o_gu.at[l, 1], True),
                  (down.at[l], o_down.at[l], False)]
    get = Fetch(items, sems)
    kinds = len(items) // layers

    def load(n):
        kind = n % kinds
        return pltpu.make_async_copy(items[n][1], (wqkv_s, wo_s, wgu_s.at[0], wgu_s.at[1], wd_s)[kind], load_sem.at[kind])

    def arrive(n):
        get.ready(n)
        load(n).start()

    def store(k, src, dst):
        return pltpu.make_async_copy(src, dst, out_sem.at[k])

    h_in = store(0, x, h_s)
    h_in.start()
    get.begin(pltpu.get_barrier_semaphore())
    vt_s[HEAD:, :] = jnp.ones((ONES, t), BF)
    on_z, on_xy, on_diagonal = get.on_z, get.on_xy, get.on_diagonal
    on_z(0)
    on_z(1)
    on_xy(0)
    on_xy(1)
    on_diagonal(0)
    on_diagonal(1)
    arrive(0)
    arrive(1)
    h_in.wait()
    stores = []

    def later(*what):
        stores.append(store(*what))
        stores[-1].start()

    for l in range(layers):
        a = l * kinds
        b = a + kinds
        more = l < layers - 1
        later(0, h_s, o_h.at[l])
        load(a).wait()

        def enter(i, l=l, a=a):
            at = span(i, RT)
            n = normed(h_s[at, :])
            cs, sn = cos[at, :], sin[at, :]
            for m in HEADS:
                q_s[at, lane(m)] = turn(mm(n, wqkv_s[:, lane(m)]).astype(BF), cs, sn)
            k_s[at, :] = turn(mm(n, wqkv_s[:, lane(2)]).astype(BF), cs, sn)
            v = mm(n, wqkv_s[:, lane(3)])
            v_s[at, :] = v.astype(BF)
            vt_s[:HEAD, at] = v.T.astype(BF)
            if l == 0:
                at_step(i, 0, (on_z, 2))
            elif l == layers - 1:
                at_step(i, 1, (on_diagonal, a + 4))

        loop(t // RT, enter)
        later(1, q_s, o_q.at[l])
        later(2, k_s, o_k.at[l])
        later(3, v_s, o_v.at[l])

        def queries(iq, l=l):
            at = span(iq, RT)
            top_s[...] = jnp.full(top_s.shape, NEG, F32)
            mix_s[...] = jnp.zeros(mix_s.shape, F32)

            def block(j, masked):
                here = span(j, RT)
                key, value = k_s[here, :], vt_s[:, here]
                scores = [mt(key, q_s[at, lane(m)]) for m in HEADS]
                weights, keeps = [], []
                for m, s in enumerate(scores):
                    if masked:
                        s = jnp.where(causal(RT), s, HIDDEN)
                    old = top_s[m : m + 1, :]
                    top = jnp.maximum(old, s.max(0, keepdims=True))
                    top_s[m : m + 1, :] = top
                    weights.append(jnp.exp2((s - top) * TEMPER).astype(BF))
                    keeps.append(jnp.exp2((old - top) * TEMPER))
                for m in HEADS:
                    mix_s[m] = mix_s[m] * keeps[m] + mm(value, weights[m])

            loop(iq, lambda j: block(j, False))
            block(iq, True)
            for m in HEADS:
                total = mix_s[m, HEAD : HEAD + 1, :]
                o_s[at, lane(m)] = (mix_s[m, :HEAD, :] * (1 / total)).T.astype(BF)
                lse_s[m : m + 1, at] = top_s[m : m + 1, :] * SCALE + jnp.log(total)
            if l == 0:
                at_step(iq, 0, (on_xy, 2))
                at_step(iq, 1, (on_z, 3), (on_diagonal, 2))
                at_step(iq, 2, (on_xy, 3))
                at_step(iq, 3, (on_z, 4), (on_diagonal, 3))

        loop(t // RT, queries)
        later(4, o_s, o_o.at[l])
        later(5, lse_s, o_lse.at[l])
        load(a + 1).wait()
        if l == 0:
            on_xy(4)
            on_z(b)
            on_z(b + 1)
            on_diagonal(4)
        if more:
            for n in range(a + 2, b):
                arrive(n)
            for n in range(a + 2, b):
                load(n).wait()

        def leave(i, l=l, b=b, more=more):
            at = span(i, RT)
            mid = h_s[at, :] + mm(o_s[at, :], wo_s[...]).astype(BF)
            mid_s[at, :] = mid
            if more:
                n = normed(mid)
                for p in range(f // FB):
                    part = slice(p * FB, (p + 1) * FB)
                    g, u = mm(n, wgu_s[0, :, part]), mm(n, wgu_s[1, :, part])
                    act_s[:, part] = (g * sigmoid(g) * u).astype(BF)
                h_s[at, :] = mid + mm(act_s[...], wd_s[...]).astype(BF)
            if l == 0:
                at_step(i, 0, (on_xy, b), (on_xy, b + 1), (on_z, b + 2))
                at_step(i, 1, (on_diagonal, b), (on_diagonal, b + 1), (on_xy, b + 2), (on_z, b + 3))
                at_step(i, 2, (on_diagonal, b + 2), (on_xy, b + 3), (on_z, b + 4))
                at_step(i, 3, (on_diagonal, b + 3), (on_xy, b + 4))

        stores[0].wait()
        loop(t // RT, leave)
        later(6, mid_s, o_mid.at[l])
        if more:
            arrive(b)
            arrive(b + 1)
        else:
            for n in range(a + 2, b):
                get.ready(n)
        for one in stores[1:]:
            one.wait()
        stores.clear()
    for n in range(len(items)):
        get.sent(n)


def forward(x, qkv, wo, gate, up, down, cos, sin):
    layers = qkv.shape[0]
    t, d = x.shape
    f = gate.shape[-1]
    n = 5 * layers
    once = lambda *dims: shape(BF, layers, *dims)
    return pl.pallas_call(
        functools.partial(forward_kernel, layers=layers),
        in_specs=[ANY] + [WHOLE] * 7,
        out_specs=[ANY] * 11,
        out_shape=[once(d, 2 * PAIR), once(PAIR, d), once(2, d, f), once(f, d), once(t, d), once(t, d), once(t, PAIR), once(t, HEAD), once(t, HEAD),
                   once(t, PAIR), shape(F32, layers, 2, t)],
        scratch_shapes=[vm(BF, t, d), vm(BF, t, d), vm(BF, t, PAIR), vm(BF, t, HEAD), vm(BF, t, HEAD), vm(BF, HEAD + ONES, t), vm(BF, t, PAIR),
                        vm(F32, 2, t), vm(F32, 2, RT), vm(F32, 2, HEAD + ONES, RT), vm(BF, RT, f), vm(BF, d, 2 * PAIR), vm(BF, PAIR, d), vm(BF, 2, d, f),
                        vm(BF, f, d), dma(5), dma(7), *fetch_sems(n)],
        compiler_params=pltpu.CompilerParams(collective_id=0, has_side_effects=True, vmem_limit_bytes=VMEM),
    )(x, qkv, wo, gate, up, down, cos, sin)


class Sums:
    def __init__(self, total, slots, own, near, right, left, out, step, sems):
        self.rep, self.dp = lax.axis_index("rep"), lax.axis_index("dp")
        self.z, self.c = self.dp // 2, self.dp % 2
        self.total, self.slots, self.own, self.near, self.right, self.left, self.out, self.step = total, slots, own, near, right, left, out, step
        (self.near_send, self.near_recv, self.right_send, self.right_recv, self.left_send, self.left_recv, self.out_sem,
         self.near_free, self.right_free, self.left_free) = sems

    def core(self, z, c):
        return (self.rep, z * 2 + c)

    def slot(self, n):
        return lax.rem(n, self.slots) if self.slots > 1 else 0

    def to_partner(self):
        return self.core(self.z, 1 - self.c)

    def reused(self, n, sem):
        pl.when(n >= self.slots)(lambda: pl.semaphore_wait(sem, 1))

    def again(self, n, sem, to):
        pl.when(n + self.slots < self.total)(lambda: signal(sem, to))

    def near_copy(self, n, j):
        k = self.slot(n)
        return remote(self.own(n, j, 1 - self.c), self.near(k, j), self.near_send.at[k, j], self.near_recv.at[k, j], self.to_partner())

    def right_copy(self, n, j):
        k = self.slot(n)
        to = self.core(jnp.minimum(self.z + 1, CHIPS - 1), self.c)
        return remote(self.own(n, j, self.c), self.right(k, j), self.right_send.at[k, j], self.right_recv.at[k, j], to)

    def left_copy(self, n, j):
        k = self.slot(n)
        to = self.core(jnp.maximum(self.z - 1, 0), self.c)
        return remote(self.own(n, j, self.c), self.left(k, j), self.left_send.at[k, j], self.left_recv.at[k, j], to)

    def add(self, to, *terms):
        lead = [(i,) for i in range(to.shape[0])] if len(to.shape) > 2 else [()]

        def some(i):
            at = span(i, self.step)
            for index in lead:
                total = to[(*index, at)].astype(F32)
                for term in terms:
                    total = total + term[(*index, at)].astype(F32)
                to[(*index, at)] = total.astype(BF)

        loop(to.shape[-2] // self.step, some)

    def exchange(self, n):
        self.reused(n, self.near_free)
        for j in range(CHIPS):
            self.near_copy(n, j).start()

    def pair(self, n):
        for j in range(CHIPS):
            self.near_copy(n, j).wait_recv()
            self.add(self.own(n, j, self.c), self.near(self.slot(n), j))
        for j in range(CHIPS):
            self.near_copy(n, j).wait_send()
        self.again(n, self.near_free, self.to_partner())

    def along(self, n, s, only=None):
        k = self.slot(n)

        @pl.when(self.z == s)
        def _():
            if not only:
                self.reused(n, self.right_free)
            for j in [j for j in range(CHIPS - 1, s, -1) if only is None or j == CHIPS - 1 - only]:
                copy = self.right_copy(n, j)
                if s:
                    copy.wait_recv()
                    self.add(self.own(n, j, self.c), self.right(k, j))
                copy.start()

        @pl.when(self.z == CHIPS - 1 - s)
        def _():
            if not only:
                self.reused(n, self.left_free)
            for j in [j for j in range(CHIPS - 1 - s) if only is None or j == only]:
                copy = self.left_copy(n, j)
                if s:
                    copy.wait_recv()
                    self.add(self.own(n, j, self.c), self.left(k, j))
                copy.start()

    def last(self, n):
        k = self.slot(n)
        for z in range(CHIPS):

            @pl.when(self.z == z)
            def _(z=z):
                terms = []
                if z > 0:
                    self.right_copy(n, z).wait_recv()
                    terms.append(self.right(k, z))
                if z < CHIPS - 1:
                    self.left_copy(n, z).wait_recv()
                    terms.append(self.left(k, z))
                self.add(self.own(n, z, self.c), *terms)
                self.result(n, z).start()
                for j in range(z + 1, CHIPS):
                    self.right_copy(n, j).wait_send()
                for j in range(z):
                    self.left_copy(n, j).wait_send()
                if z > 0:
                    self.again(n, self.right_free, self.core(z - 1, self.c))
                if z < CHIPS - 1:
                    self.again(n, self.left_free, self.core(z + 1, self.c))

    def result(self, n, z):
        return pltpu.make_async_copy(self.own(n, z, self.c), self.out(n), self.out_sem.at[self.slot(n)])

    def flush(self, n):
        self.result(n, self.z).wait()


def sum_sems(slots):
    return [dma(slots, CHIPS)] * 6 + [dma(slots)] + [pltpu.SemaphoreType.REGULAR] * 3


GU_SLOTS = 3


def back_kernel(*refs, layers, parts):
    it = iter(refs)
    take = lambda n: [next(it) for _ in range(n)]
    dy, mids, hs, os, qs, ks, vs, lses, cos, sin, w_qkv, w_o, w_gu, w_d = take(14)
    o_gu, o_d, o_wo, o_qkv = take(4)
    (dy_s, mid_s, h_s, b_s, db_s, act_s, dg_s, du_s, o_s, k_s, v_s, cos_s, sin_s, lse_s, delta_s, dq_s, wgu_s, wd_s, wo_s, wqkv_s) = take(20)
    own = take(4)
    near, right, left = take(4), take(4), take(4)
    sems = [take(10) for _ in range(4)]
    in_sem, w_sem = take(2)
    g_gu, g_d, g_wo, g_qkv = own

    t, d = dy_s.shape
    rep, dp = lax.axis_index("rep"), lax.axis_index("dp")
    z, c = dp // 2, dp % 2
    of = lambda i: layers - 1 - i

    def of_part(n):
        return of(n // parts), span(lax.rem(n, parts), FB)

    def out_gu(n):
        l, at = of_part(n)
        return o_gu.at[l, :, :, at]

    def flat(k, out, step):
        size = own[k].shape[1] // (2 * CHIPS)
        copies = own[k].shape[0]
        return Sums(layers, 1, lambda n, j, cc: own[k].at[n % copies, rows((2 * j + cc) * size, size), :], lambda s, j: near[k].at[j],
                    lambda s, j: right[k].at[j - 1], lambda s, j: left[k].at[j], lambda n: out.at[of(n)], step, sems[k])

    gu = Sums(layers * parts, GU_SLOTS, lambda n, j, cc: g_gu.at[lax.rem(n, GU_SLOTS), :, j, cc], lambda s, j: near[0].at[s, j],
              lambda s, j: right[0].at[s, j - 1], lambda s, j: left[0].at[s, j], out_gu, 80, sems[0])
    down, wo, qkv = flat(1, o_d, 64), flat(2, o_wo, 64), flat(3, o_qkv, 80)

    barrier = pltpu.get_barrier_semaphore()
    signal(barrier, (rep, z * 2 + 1 - c))
    pl.when(z > 0)(lambda: signal(barrier, (rep, jnp.maximum(dp - 2, 0))))
    pl.when(z < CHIPS - 1)(lambda: signal(barrier, (rep, jnp.minimum(dp + 2, 2 * CHIPS - 1))))

    def fetch(i):
        l = of(i)
        pairs = ((mids, mid_s), (hs, h_s), (os, o_s), (qs, du_s), (ks, k_s), (vs, v_s), (lses, lse_s), (w_o, wo_s), (w_qkv, wqkv_s))
        names = ("mid", "h", "o", "q", "k", "v", "lse", "wo", "wqkv")
        return {name: (src.at[l], dst, in_sem.at[n]) for n, (name, (src, dst)) in enumerate(zip(names, pairs))}

    def start(i, *names):
        for name in names:
            pltpu.make_async_copy(*fetch(i)[name]).start()

    def wait(i, *names):
        for name in names:
            pltpu.make_async_copy(*fetch(i)[name]).wait()

    def part_weights(n):
        l, at = of_part(n)
        k = lax.rem(n, 2)
        return [pltpu.make_async_copy(w_gu.at[l, :, :, at], wgu_s.at[k], w_sem.at[k, 0]), pltpu.make_async_copy(w_d.at[l, at, :], wd_s.at[k], w_sem.at[k, 1])]

    once = [pltpu.make_async_copy(src, dst, w_sem.at[2, n]) for n, (src, dst) in enumerate(((dy, dy_s), (cos, cos_s), (sin, sin_s)))]
    start(0, "mid")
    for one in [once[0]] + part_weights(0) + once[1:]:
        one.start()
    start(0, "o", "k", "v", "lse", "h", "wo", "wqkv")
    pl.semaphore_wait(barrier, 1 + jnp.where(z > 0, 1, 0) + jnp.where(z < CHIPS - 1, 1, 0))
    for one in once:
        one.wait()

    def layer(i):
        wait(i, "mid")

        def enter(r):
            at = span(r, RT)
            b_s[at, :] = normed(mid_s[at, :])
            db_s[at, :] = jnp.zeros((RT, d), F32)

        loop(t // RT, enter)

        def part(p):
            n = i * parts + p
            k = lax.rem(n, 2)
            for one in part_weights(n):
                one.wait()

            @pl.when(n + 1 < layers * parts)
            def _():
                for one in part_weights(n + 1):
                    one.start()

            def when(step, r, least, *todo):
                at_step(jnp.where(p >= least, step, -1), r, *todo)

            def before(step, r, which, *todo):
                at_step(jnp.where((p == which) & (i > 0), step, -1), r, *todo)

            def some(r):
                at = span(r, RT)
                b, dy = b_s[at, :], dy_s[at, :]
                gate, up = mm(b, wgu_s[k, 0]), mm(b, wgu_s[k, 1])
                da = mt(dy, wd_s[k]).astype(BF).astype(F32)
                sig = sigmoid(gate)
                s = gate * sig
                act_s[at, :] = (s * up).astype(BF)
                du = (da * s).astype(BF)
                dg = (da * up * (sig + s * (1 - sig))).astype(BF)
                du_s[at, :] = du
                dg_s[at, :] = dg
                db_s[at, :] += mt(dg, wgu_s[k, 0]) + mt(du, wgu_s[k, 1])
                when(r, 0, 1, (gu.pair, n - 1), (gu.along, n - 1, 0))
                when(r, 0, 2, (gu.along, n - 2, 1))
                when(r, 2, 3, (gu.last, n - 3))
                when(r, 3, 3, (gu.flush, n - 3))
                before(r, 0, 0, (qkv.pair, i - 1), (qkv.along, i - 1, 0), (down.along, i - 1, 2))
                before(r, 0, 1, (down.flush, i - 1))
                before(r, 2, 1, (wo.along, i - 1, 2), (qkv.along, i - 1, 1))
                before(r, 0, 2, (qkv.along, i - 1, 2), (wo.flush, i - 1))
                before(r, 2, 2, (qkv.last, i - 1))
                before(r, 3, 2, (qkv.flush, i - 1))

            loop(t // RT, some)
            slot = lax.rem(n, GU_SLOTS)
            for q in range(FB // HEAD):
                for which, by in enumerate((dg_s, du_s)):
                    g_gu[slot, which, :, :, :, lane(q)] = tm(b_s[...], by[:, lane(q)]).astype(BF).reshape(CHIPS, 2, d // (2 * CHIPS), HEAD)
                g_d[i % 2, span(p * (FB // HEAD) + q, HEAD), :] = tm(act_s[:, lane(q)], dy_s[...]).astype(BF)
            gu.exchange(n)
            when(0, 0, 2, (gu.along, n - 2, 2))
            before(0, 0, 0, (down.last, i - 1), (wo.along, i - 1, 1))
            before(0, 0, 1, (wo.last, i - 1))

        loop(parts, part)
        n = i * parts + parts - 1

        start(i, "q")
        wait(i, "o", "k", "v", "lse", "wo")

        def leave(r):
            at = span(r, RT)
            dmid = (dy_s[at, :].astype(F32) + normed_back(mid_s[at, :], db_s[at, :].astype(BF).astype(F32))).astype(BF)
            dy_s[at, :] = dmid
            for m in HEADS:
                do = mt(dmid, wo_s[lane(m), :]).astype(BF)
                act_s[at, lane(m)] = do
                delta_s[m : m + 1, at] = (do.astype(F32) * o_s[at, lane(m)].astype(F32)).T.sum(0, keepdims=True)
            at_step(r, 0, (gu.pair, n), (gu.along, n, 0), (gu.along, n - 1, 1), (down.exchange, i))
            at_step(r, 3, (gu.last, n - 2))

        loop(t // RT, leave)
        g_wo[0] = tm(o_s[...], dy_s[...]).astype(BF)
        gu.flush(n - 2)
        wo.exchange(i)
        down.pair(i)
        down.along(i, 0)
        pl.when(i < layers - 1)(lambda: start(i + 1, "o", "mid"))

        db_s[:, :PAIR] = jnp.zeros((t, PAIR), F32)
        wait(i, "q")

        def queries(iq):
            at = span(iq, RT)
            dq_s[...] = jnp.zeros_like(dq_s)

            def block(j, masked):
                here = span(j, RT)
                key, value = k_s[here, :], v_s[here, :]
                dk, dv = db_s[here, lane(0)], db_s[here, lane(1)]
                for m in HEADS:
                    q, do = du_s[at, lane(m)], act_s[at, lane(m)]
                    p = jnp.exp2(mt(key, q) * TEMPER - lse_s[m : m + 1, at] * LOG2E)
                    if masked:
                        p = jnp.where(causal(RT), p, 0.0)
                    ds = (p * (mt(value, do) - delta_s[m : m + 1, at])).astype(BF)
                    dv += mm(p.astype(BF), do)
                    dk += mm(ds, q)
                    dq_s[:, lane(m)] += tm(ds, key)
                db_s[here, lane(0)] = dk
                db_s[here, lane(1)] = dv

            loop(iq, lambda j: block(j, False))
            block(iq, True)
            dg_s[at, :] = (dq_s[...] * SCALE).astype(BF)
            at_step(iq, 1, (gu.along, n - 1, 2))
            at_step(iq, 2, (gu.along, n, 1), (wo.pair, i), (wo.along, i, 0), (gu.last, n - 1))
            at_step(iq, 3, (gu.flush, n - 1), (down.along, i, 1, 0))

        loop(t // RT, queries)
        wait(i, "h", "wqkv")

        def leave_qkv(r):
            at = span(r, RT)
            cs, sn = cos_s[at, :], sin_s[at, :]
            for m in HEADS:
                dg_s[at, lane(m)] = turn_back(dg_s[at, lane(m)], cs, sn)
            act_s[at, lane(0)] = turn_back((db_s[at, lane(0)] * SCALE).astype(BF), cs, sn)
            act_s[at, lane(1)] = db_s[at, lane(1)].astype(BF)
            h = h_s[at, :]
            b_s[at, :] = normed(h)
            da = (mt(dg_s[at, :], wqkv_s[:, :PAIR]) + mt(act_s[at, :], wqkv_s[:, PAIR:])).astype(BF).astype(F32)
            dy_s[at, :] = (dy_s[at, :].astype(F32) + normed_back(h, da)).astype(BF)
            at_step(r, 1, (gu.along, n, 2))

        loop(t // RT, leave_qkv)
        for m in HEADS:
            g_qkv[0, :, lane(m)] = tm(b_s[...], dg_s[:, lane(m)]).astype(BF)
            g_qkv[0, :, lane(m + 2)] = tm(b_s[...], act_s[:, lane(m)]).astype(BF)
        qkv.exchange(i)
        down.along(i, 1, 1)
        gu.last(n)
        gu.flush(n)
        pl.when(i < layers - 1)(lambda: start(i + 1, "k", "v", "lse", "h", "wo", "wqkv"))

    loop(layers, layer)
    n = layers - 1
    qkv.pair(n)
    qkv.along(n, 0)
    down.along(n, 2)
    wo.along(n, 1)
    down.last(n)
    wo.along(n, 2)
    qkv.along(n, 1, 0)
    qkv.along(n, 1, 1)
    qkv.along(n, 2)
    wo.last(n)
    qkv.last(n)
    for one in (down, wo, qkv):
        one.flush(n)


def backward(dy, mids, hs, os, qs, ks, vs, lses, cos, sin, w_qkv, w_o, w_gu, w_d):
    layers, t, d = mids.shape
    f = w_d.shape[1]
    parts = f // FB
    flats = [(f, d), (PAIR, d), (d, 2 * PAIR)]
    part = lambda rows, width: (rows // (2 * CHIPS), width)
    blocks = lambda n: [vm(BF, GU_SLOTS, n, 2, *part(d, FB))] + [vm(BF, n, *part(*dims)) for dims in flats]
    scratch = [vm(BF, t, d)] * 4 + [vm(F32, t, d)] + [vm(BF, t, FB)] * 4 + [vm(BF, t, HEAD)] * 2 + [vm(F32, t, HALF)] * 2
    scratch += [vm(F32, 2, t)] * 2 + [vm(F32, RT, PAIR), vm(BF, 2, 2, d, FB), vm(BF, 2, FB, d), vm(BF, PAIR, d), vm(BF, d, 2 * PAIR)]
    scratch += [vm(BF, GU_SLOTS, 2, CHIPS, 2, *part(d, FB)), vm(BF, 2, f, d), vm(BF, 1, PAIR, d), vm(BF, 1, d, 2 * PAIR)]
    scratch += blocks(CHIPS) + blocks(CHIPS - 1) + blocks(CHIPS - 1)
    for slots in (GU_SLOTS, 1, 1, 1):
        scratch += sum_sems(slots)
    scratch += [dma(9), dma(3, 3)]
    given = [dy, mids, hs, os, qs, ks, vs, lses, cos, sin, w_qkv, w_o, w_gu, w_d]
    mine = lambda rows, width: shape(BF, layers, *part(rows, width))
    return pl.pallas_call(
        functools.partial(back_kernel, layers=layers, parts=parts),
        in_specs=[ANY] * len(given),
        out_specs=[ANY] * 4,
        out_shape=[shape(BF, layers, 2, *part(d, f))] + [mine(*dims) for dims in flats],
        scratch_shapes=scratch,
        compiler_params=pltpu.CompilerParams(collective_id=1, has_side_effects=True, vmem_limit_bytes=VMEM),
    )(*given)


def adamw(w, m, v, g):
    m = 0.9 * m + 0.1 * g
    v = 0.95 * v + 0.05 * g * g
    step = m * lax.rsqrt(v + 1e-8) + 0.1 * w
    return (w - 0.02 * step).astype(BF), m, v


def tables(tokens):
    angle = jnp.arange(tokens, dtype=F32)[:, None] * THETA ** (-jnp.arange(HALF, dtype=F32) / HALF)
    return jnp.cos(angle), jnp.sin(angle)


def solution(mesh):
    def step(x, dy, *arrays):
        weights, m, v = (arrays[i : i + 7] for i in (0, 7, 14))
        wq, wk, wv, wo, w_gate, w_up, w_down = weights
        x, dy = x[0], dy[0]
        cos, sin = tables(x.shape[0])
        w_qkv, w_o, w_gu, w_d, h, mid, q, k, v_, o, lse = forward(x, jnp.concatenate([wq, wk, wv], axis=2), wo, w_gate, w_up, w_down, cos, sin)
        gu, down, by_wo, qkv = backward(dy, mid, h, o, q, k, v_, lse, cos, sin, w_qkv, w_o, w_gu, w_d)
        gradients = [*jnp.split(qkv, (PAIR, PAIR + HEAD), axis=2), by_wo, gu[:, 0], gu[:, 1], down]
        new = [adamw(w.astype(F32), m, v, g.astype(F32)) for w, m, v, g in zip(weights, m, v, gradients, strict=True)]
        return tuple(one[which] for which in range(3) for one in new)

    states, cut = P(("rep", "dp"), None, None), P(None, "dp", None)
    return jax.shard_map(
        step,
        mesh=mesh,
        in_specs=(states, states) + (cut,) * 21,
        out_specs=(P("rep", "dp", None),) * 21,
        check_vma=False,
    )
```
